32 devices in a mesh: mem: 4 (over x, core), reg: 8 (over z, y).
Axes of the slice: x: 2, y: 2, z: 4, core: 2. Of those that a mesh axis runs over, the one named last changes fastest.
Arguments:
- profiles: bfloat16 [2048, 80, 127], P('reg', 'mem'), may hold values from -6 to 6
- jacobian: bfloat16 [2048, 16, 127], P('reg'), may hold values from -0.5 to 0.5
- departure: float32 [32768], P('reg'), may hold values from -6 to 6
- obs_rinv: float32 [32768], P('reg'), may hold values from 0.1 to 2
- obs_level: int32 [32768], P('reg'), may hold values from 0 to 126
- vertical_modes: float32 [127, 12], replicated, may hold values from -2 to 2
- send_rows: int32 [8, 7, 512], P('reg'), may hold values from -1 to 4095, as said below
- counts: int32 [8, 7], P('reg'), may hold values from 64 to 512, as said below
- loc_taper: float32 [8, 7, 512], P('reg'), may hold values from 0.05 to 1
Outputs:
- gram_matrices: float32 [8, 960, 960], P('reg', 'mem')
- weighted_departures: float32 [8, 960], P('reg', 'mem')
The draws below stay inside these ranges and needn't reach their ends.
Inputs may be any that keep to these rules, and one draw needn't show every extreme that they name: counts[s, d] of the 512 slots that owner s sends to region (s + d - 3) mod 8 are live, the first ones; in every draw one region has all 512 slots live from each of its 7 owners. `send_rows`: a live slot holds a row of the owner's 4096 observations, no row twice within one (s, d); the other slots hold -1.
All inputs are finite; a program needn't handle non-finite values.
Results may differ from the reference program's by a relative error of at most 0.0095.
Values may be sent and summed in bfloat16 or wider, within the bound.
A program may use at most 64 MiB of HBM per device.

```python
import math
import jax
import jax.numpy as jnp
from jax import lax

ENS = 80
MODES = 12
LEV = 127
CH = 16
HALF = 3
COLS = 256
CAP = 512
REGIONS = 8
NB = 7
OBS = 32768
COLS_ALL = 2048


def routing_tables(key):
    key_base = jax.random.fold_in(key, 11)
    key_density = jax.random.fold_in(key, 12)
    key_full = jax.random.fold_in(key, 13)
    key_rows = jax.random.fold_in(key, 14)
    base_count = jax.random.randint(key_base, (REGIONS, NB), CAP // 8, CAP // 2 + 1)
    density = jax.random.randint(key_density, (REGIONS,), 1, 4)
    source = jnp.arange(REGIONS, dtype=jnp.int32)[:, None]
    offset = jnp.arange(NB, dtype=jnp.int32)[None, :]
    target = (source + offset - HALF) % REGIONS
    count_table = jnp.minimum(base_count * density[target], CAP)
    full_region = jax.random.randint(key_full, (), 0, REGIONS)
    count_table = jnp.where(target == full_region, CAP, count_table).astype(jnp.int32)
    row_keys = jax.random.split(key_rows, REGIONS * NB)
    orders = jax.vmap(lambda single: jax.random.permutation(single, COLS * CH)[:CAP])(row_keys)
    orders = orders.reshape(REGIONS, NB, CAP).astype(jnp.int32)
    slot_ids = jnp.arange(CAP, dtype=jnp.int32)[None, None, :]
    listed = jnp.where(slot_ids < count_table[:, :, None], orders, -1).astype(jnp.int32)
    return (listed, count_table)


def draw_send_rows(key, part):
    listed, count_table = routing_tables(key)
    return listed


def draw_counts(key, part):
    listed, count_table = routing_tables(key)
    return count_table


def plant(array, stream_key, smallest, high):
    spot = [jax.random.randint(jax.random.fold_in(stream_key, axis), (), 0, length) for axis, length in enumerate(array.shape)]
    widest = array.shape.index(max(array.shape))
    beside = spot[:widest] + [(spot[widest] + 1) % array.shape[widest]] + spot[widest + 1:]
    return array.at[tuple(spot)].set(smallest).at[tuple(beside)].set(high)


def level_of(stream_key, dims, cuts, least, largest):
    factor_of = 1.0
    for dim, shards_of in cuts:
        steps = jax.random.uniform(jax.random.fold_in(jax.random.fold_in(stream_key, 6), dim), (shards_of,), jnp.float32, least / len(cuts), largest / len(cuts))
        factor_of = factor_of * jnp.repeat(jnp.exp(steps), dims[dim] // shards_of).reshape((-1,) + (1,) * (len(dims) - 1 - dim))
    return factor_of


def noise(rng, dims, deviation, most, shards=(), kind=jnp.bfloat16):
    result = jax.random.normal(rng, dims, jnp.float32) * deviation
    if len(shards) > 0:
        result = level_of(rng, dims, shards, -0.22, 0.18) * result
    return jnp.clip(result, min=-most, max=most).astype(kind)


def setup_inputs(seed: int = 0) -> dict:
    seeds = jax.random.split(jax.random.key(seed), 10)
    profiles = noise(seeds[0], (COLS_ALL, ENS, LEV), 1.0, 6.0, ((0, 8), (1, 4)))
    jacobian = noise(seeds[1], (COLS_ALL, CH, LEV), LEV ** -0.5, 0.5, ((0, 8),))
    departure = noise(seeds[2], (OBS,), 1.0, 6.0, ((0, 8),), jnp.float32)
    obs_rinv = jnp.clip(jnp.exp(math.log(2.0) - 2.9957323 * jax.random.uniform(seeds[3], (OBS,), jnp.float32) ** level_of(seeds[3], (OBS,), ((0, 8),), -0.2, 0.2)), 0.1, 2.0)
    obs_level = plant(jax.random.randint(seeds[4], (OBS,), 0, LEV), jax.random.fold_in(seeds[4], 1), 0, LEV - 1).astype(jnp.int32)
    vertical_modes = noise(seeds[5], (LEV, MODES), 0.3, 2.0, (), jnp.float32)
    send_rows = draw_send_rows(jax.random.fold_in(seeds[9], 71), 0)
    counts = draw_counts(jax.random.fold_in(seeds[9], 71), 0)
    loc_taper = jnp.clip(0.05 + 0.95 * jax.random.uniform(seeds[8], (REGIONS, NB, CAP), jnp.float32) ** level_of(seeds[8], (REGIONS, NB, CAP), ((0, 8),), -0.2, 0.2), 0.05, 1.0)
    return {"profiles": profiles, "jacobian": jacobian, "departure": departure, "obs_rinv": obs_rinv, "obs_level": obs_level, "vertical_modes": vertical_modes, "send_rows": send_rows, "counts": counts, "loc_taper": loc_taper}


def reference(profiles, jacobian, departure, obs_rinv, obs_level, vertical_modes, send_rows, counts, loc_taper):
    profile_blocks = profiles.reshape(REGIONS, COLS, ENS, LEV)
    jacob_blocks = jacobian.reshape(REGIONS, COLS, CH, LEV)

    def owner_pert(operands):
        profile_one, jacob_one = operands
        values = jnp.einsum('cql,cml->mcq', jacob_one.astype(jnp.float32), profile_one.astype(jnp.float32), precision=lax.Precision.HIGHEST)
        return values.reshape(ENS, COLS * CH).astype(jnp.bfloat16)

    all_pert = lax.map(owner_pert, (profile_blocks, jacob_blocks))
    all_pert = jnp.transpose(all_pert, (1, 0, 2)).reshape(ENS, REGIONS * COLS * CH)
    factor = (ENS - 1) ** -0.5
    offsets = jnp.arange(NB, dtype=jnp.int32)
    slot_ids = jnp.arange(CAP, dtype=jnp.int32)

    def one_region(region):
        source = (region - offsets + HALF) % REGIONS
        listed = send_rows[source, offsets]
        live_slot = slot_ids[None, :] < counts[source, offsets][:, None]
        picked = jnp.where(live_slot, listed, 0)
        global_ids = (source[:, None] * (COLS * CH) + picked).reshape(-1)
        weight32 = jnp.where(live_slot, obs_rinv[global_ids].reshape(NB, CAP) * loc_taper[source, offsets], 0.0).reshape(-1)
        weight = weight32.astype(jnp.bfloat16)
        dep_weighted = (weight32 * departure[global_ids]).astype(jnp.bfloat16)
        mode_values = (vertical_modes[obs_level[global_ids]].T * factor).astype(jnp.bfloat16)
        region_pert = all_pert[:, global_ids]
        modulated = (region_pert.astype(jnp.float32)[:, None, :] * mode_values.astype(jnp.float32)[None, :, :]).astype(jnp.bfloat16)
        modulated = modulated.reshape(ENS * MODES, NB * CAP)
        weighted = (modulated.astype(jnp.float32) * weight.astype(jnp.float32)[None, :]).astype(jnp.bfloat16)
        gram_block = jnp.dot(modulated.astype(jnp.float32), weighted.astype(jnp.float32).T, precision=lax.Precision.HIGHEST)
        dep_block = jnp.dot(modulated.astype(jnp.float32), dep_weighted.astype(jnp.float32), precision=lax.Precision.HIGHEST)
        return gram_block, dep_block

    gram_matrices, weighted_departures = lax.map(one_region, jnp.arange(REGIONS, dtype=jnp.int32))
    return (gram_matrices, weighted_departures)
```

```python
import functools

import jax
import jax.numpy as jnp
from jax import lax
from jax.experimental import pallas as pl
from jax.experimental.pallas import tpu as pltpu
from jax.sharding import PartitionSpec as P

ENS = 80
LANE = 128
SUB = 8
GROUP = 16
NT = (((1,), (1,)), ((), ()))
VMEM = pl.BlockSpec(memory_space=pltpu.VMEM)
HBM = pl.BlockSpec(memory_space=pltpu.MemorySpace.HBM)
MESH = pl.DeviceIdType.MESH


def iota(shape, dim):
    return lax.broadcasted_iota(jnp.int32, shape, dim)


def hot(mask):
    return jnp.where(mask, 1.0, 0.0).astype(jnp.bfloat16)


def times(left, right):
    return jnp.dot(left, right, preferred_element_type=jnp.float32)


def merge(a, b, bit, s, u):
    up = pltpu.roll(a, SUB - bit, 0)
    if b is None:
        return jnp.where((u & bit) != 0, up, a)
    low = (s & bit) == 0
    if 2 * bit == SUB:
        same = (s & bit) == (u & bit)
        return jnp.where(same, jnp.where(low, a, b), pltpu.roll(jnp.where(low, b, a), bit, 0))
    down = pltpu.roll(b, bit, 0)
    return jnp.where((u & bit) != 0, jnp.where(low, up, b), jnp.where(low, a, down))


def diagonal(parts, s, u):
    fours = [merge(parts[i], parts[i + 4] if len(parts) > 4 else None, 4, s, u) for i in range(4)]
    twos = [merge(fours[i], fours[i + 2], 2, s, u) for i in range(2)]
    return merge(twos[0], twos[1], 1, s, u)


def turn_jacobian(jac, wide, turned):
    levels, channels, cols = jac.shape
    pitch = wide.shape[1] // channels
    for l in range(levels):
        line = jac[l].astype(jnp.float32)
        for half in range(cols // LANE):
            for q in range(0, channels, SUB):
                part = line[q : q + SUB, half * LANE : (half + 1) * LANE]
                wide[half, pl.ds(q * pitch + l, SUB, stride=pitch), :] = part
    for half in range(cols // LANE):
        for q in range(channels):
            plane = wide[half, q * pitch : q * pitch + LANE, :]
            turned[q, half * LANE : (half + 1) * LANE, :] = plane.T[:, :levels].astype(jnp.bfloat16)


def side_rows(me, rinv, dep, level, modes, padded, extra, share):
    kinds, levels = modes.shape
    lanes = extra.shape[1]
    padded[...] = jnp.zeros_like(padded)
    padded[share : share + kinds, :] = modes[...] * ((ENS - 1) ** (-0.5))
    mine = padded[pl.ds(me * share, SUB), :].astype(jnp.bfloat16)
    s = iota((SUB, lanes), 0)
    holds_dep = (s == SUB - share + kinds % share) & (me == kinds // share)
    for g in range(extra.shape[0] // SUB):
        at = slice(g * lanes, (g + 1) * lanes)
        root = jnp.sqrt(rinv[:, at])
        high = root.astype(jnp.bfloat16).astype(jnp.float32)
        found = times(mine, hot(iota((levels, lanes), 0) == level[:, at]))
        found = jnp.where(holds_dep, dep[:, at] * root, found)
        found = jnp.where(s == 0, high, jnp.where(s == 1, root - high, found))
        extra[g * SUB : (g + 1) * SUB, :] = found
    channels = lanes // GROUP
    source, target = iota((lanes, lanes), 0), iota((lanes, lanes), 1)
    swap = hot(target == (source % channels) * GROUP + source // channels)
    extra[...] = times(extra[...].astype(jnp.bfloat16), swap)


def fill_table(prof, turned, extra, table):
    members, cols, levels = prof.shape
    groups, height, lanes = table.shape
    s, lane = iota((SUB, lanes), 0), iota((SUB, lanes), 1)
    u = lane % SUB
    upper = (lane // SUB) % 2 == 1

    def fill(g, carry):
        first = pl.ds(pl.multiple_of(g * GROUP, GROUP), GROUP)
        left = prof[:, first, :].reshape(members * GROUP, levels)
        right = turned[:, first, :].reshape(lanes, levels)
        full = lax.dot_general(left, right, NT, preferred_element_type=jnp.float32)
        parts = []
        for m in range(members):
            x = m * GROUP
            parts.append(jnp.where(upper, full[x + SUB : x + 2 * SUB], full[x : x + SUB]))
        more = extra[pl.ds(pl.multiple_of(g * SUB, SUB), SUB), :]
        root = more[0:1] + more[1:2]
        rows = [diagonal(parts[m : m + SUB], s, u) * root for m in range(0, members, SUB)]
        rows[-1] = jnp.where(s < members % SUB, rows[-1], more)
        table[g] = jnp.concatenate(rows, axis=0).astype(jnp.bfloat16)
        return carry

    lax.fori_loop(0, groups, fill, 0, unroll=4)


def gather_kernel(
    members, kinds, share, prof_h, jac_h, dep_h, rinv_h, level_h, modes_h, rows_h, counts_h, taper_h, acc,
    prof, jac, dep, rinv, level, modes, rows, counts, taper,
    padded, wide, turned, extra, table, picks, mine, region,
    s_in, s_reg, r_reg, s_hand, r_hand,
):
    blocks, height, capacity = mine.shape
    middle = blocks // 2
    n_mem, n_reg = lax.axis_size("mem"), lax.axis_size("reg")
    me, reg = lax.axis_index("mem"), lax.axis_index("reg")
    chips = n_mem // 2
    groups, _, lanes = table.shape
    channels = lanes // GROUP
    partner = {"mem": me + 1 - 2 * (me % 2), "reg": reg}
    pairs = [
        (level_h, level), (modes_h, modes), (rinv_h, rinv), (dep_h, dep), (rows_h, rows),
        (counts_h, counts), (taper_h, taper), (jac_h, jac), (prof_h, prof),
    ]
    loads = [pltpu.make_async_copy(h, v, s_in.at[i]) for i, (h, v) in enumerate(pairs)]
    for load in loads:
        load.start()

    def target(d, c):
        to = lax.rem(reg + d - middle + n_reg, n_reg)
        return {"mem": lax.rem(me + 2 * c, n_mem), "reg": to}

    def remote(src, dst, send, recv, device):
        return pltpu.make_async_remote_copy(
            src_ref=src, dst_ref=dst, send_sem=send, recv_sem=recv,
            device_id=device, device_id_type=MESH,
        )

    def across(d, c):
        return remote(mine.at[d], region.at[d, me], s_reg.at[d, c], r_reg.at[d, c], target(d, c))

    def hand(d, c):
        at = region.at[d, lax.rem(me - 2 * c + n_mem, n_mem)]
        return remote(at, at, s_hand.at[d, c], r_hand.at[d, c], partner)

    barrier = pltpu.get_barrier_semaphore()
    greeted = [target(d, c) for d in range(blocks) for c in range(chips) if (d, c) != (middle, 0)]
    greeted.append(partner)
    for device in greeted:
        pl.semaphore_signal(barrier, inc=1, device_id=device, device_id_type=MESH)

    at = lax.rem(middle - reg + n_reg, n_reg)
    lead = jnp.where(at < blocks, at, 0)

    def sent(k):
        return lax.rem(lead + k, blocks)

    def taken(k):
        return blocks - 1 - sent(k)

    for load in loads[:4]:
        load.wait()
    side_rows(me, rinv, dep, level, modes, padded, extra, share)
    for load in loads[4:7]:
        load.wait()

    def placed(d):
        live = iota((1, capacity), 1) < counts[0, d]
        return live, jnp.where(live, rows[d], 0)

    for d in range(blocks):
        _, picked = placed(d)
        low = (picked % channels) * GROUP + (picked // channels) % GROUP
        picks[d] = hot(iota((lanes, capacity), 0) == low)

    loads[7].wait()
    turn_jacobian(jac, wide, turned)
    loads[8].wait()
    fill_table(prof, turned, extra, table)

    s = iota((height, capacity), 0)
    is_dep = (s == members + kinds % share) & (me == kinds // share)
    for k in range(blocks):
        d = sent(k)
        live, picked = placed(d)
        high = picked // lanes
        found = times(table[...].reshape(groups * height, lanes), picks[d])
        chosen = found[:height]
        for h in range(1, groups):
            chosen = jnp.where(high == h, found[h * height : (h + 1) * height], chosen)
        root = jnp.sqrt(jnp.where(live, taper[d], 0.0))
        block = (chosen * jnp.where((s < members) | is_dep, root, 1.0)).astype(jnp.bfloat16)
        mine[d] = block
        if k == 0:
            pl.semaphore_wait(barrier, len(greeted))

        @pl.when(d == middle)
        def _():
            region[middle, me] = block

        @pl.when(d != middle)
        def _():
            across(d, 0).start()

        for c in range(1, chips):
            across(d, c).start()

    acc[...] = jnp.zeros_like(acc)
    size = members * kinds
    wide_rows = n_mem * height
    row, col = iota((2 * size, wide_rows), 0), iota((2 * size, wide_rows), 1)
    kind = row % kinds
    own = me * height + row // kinds
    spread = hot(col == jnp.where(row < size, own, (kind // share) * height + members + kind % share))

    def forward(k):
        d = taken(k)

        @pl.when(d != middle)
        def _():
            across(d, 0).wait_recv()

        hand(d, 0).start()
        for c in range(1, chips):
            across(d, c).wait_recv()
            hand(d, c).start()

    def multiply(k):
        d = taken(k)
        for c in range(chips):
            hand(d, c).wait_recv()
        parts = [region[d, j].astype(jnp.float32) for j in range(n_mem)]
        every = jnp.concatenate(parts, axis=0).astype(jnp.bfloat16)
        both = times(spread, every)
        own = (both[:size] * both[size:]).astype(jnp.bfloat16)
        lines = []
        for l in range(kinds):
            at = members + l % share
            line = jnp.broadcast_to(parts[l // share][at : at + 1], (GROUP, capacity))
            line = line.astype(jnp.bfloat16)
            lines.append(every * jnp.concatenate([line] * (wide_rows // GROUP), axis=0))
        lines.append(every[wide_rows - 2 * GROUP :])
        left = jnp.concatenate(lines, axis=0)
        acc[...] += lax.dot_general(left, own, NT, preferred_element_type=jnp.float32)

    def step(k, carry):
        @pl.when(k < blocks)
        def _():
            forward(k)

        @pl.when(k >= 1)
        def _():
            multiply(k - 1)

        return carry

    lax.fori_loop(0, blocks + 1, step, 0)
    for d in range(blocks):
        for c in range(chips):
            if (d, c) != (middle, 0):
                across(d, c).wait_send()
            hand(d, c).wait_send()


def write_kernel(members, kinds, n_mem, height, dep_row, acc, gram, depart, rows, out, out_dep, sems):
    size = members * kinds
    total = size * n_mem
    for t in range(-(-size // LANE)):
        wide = min(LANE, size - t * LANE)
        for l in range(kinds):
            for j in range(n_mem):
                at = (l * n_mem + j) * height
                part = acc[at : at + members, t * LANE : t * LANE + wide]
                to = pl.ds(j * size + l, members, stride=kinds)
                rows[t, to, 0:wide] = part
    out_dep[...] = acc[dep_row : dep_row + 1, :]
    pltpu.make_async_copy(out_dep, depart, sems.at[0]).start()
    copies = []
    for i in range(-(-total // LANE)):
        tall = min(LANE, total - i * LANE)
        at = slice(i * LANE, i * LANE + tall)
        for t in range(-(-size // LANE)):
            wide = min(LANE, size - t * LANE)
            turned = rows[t, at, :].T
            out[0, t * LANE : t * LANE + wide, at] = turned[:wide]
        copy = pltpu.make_async_copy(out.at[:, :, at], gram.at[:, :, at], sems.at[1 + i])
        copy.start()
        copies.append(copy)
    pltpu.make_async_copy(out_dep, depart, sems.at[0]).wait()
    for copy in copies:
        copy.wait()


def local(
    profiles, jacobian, departure, obs_rinv, obs_level, vertical_modes, send_rows, counts, loc_taper
):
    cols, members, levels = profiles.shape
    channels = jacobian.shape[1]
    blocks, capacity = send_rows.shape[1], send_rows.shape[2]
    kinds = vertical_modes.shape[1]
    n_mem = lax.axis_size("mem")
    chips = n_mem // 2
    share = -(-(kinds + 1) // n_mem)
    height = members + share
    size = members * kinds
    lanes = GROUP * channels
    dma = pltpu.SemaphoreType.DMA
    args = (
        profiles.transpose(1, 0, 2), jacobian.transpose(2, 1, 0),
        departure[None], obs_rinv[None], obs_level[None], vertical_modes.T,
        send_rows.transpose(1, 0, 2), counts, loc_taper.transpose(1, 0, 2),
    )
    args = [pltpu.with_memory_space_constraint(a, pltpu.MemorySpace.HBM) for a in args]
    buffers = [pltpu.VMEM(a.shape, a.dtype) for a in args]
    buffers[7] = pltpu.SMEM(counts.shape, counts.dtype)
    pitch = -(-levels // LANE) * LANE + 1
    acc_rows = kinds * n_mem * height + 2 * GROUP
    acc = pl.pallas_call(
        functools.partial(gather_kernel, members, kinds, share),
        out_shape=jax.ShapeDtypeStruct((acc_rows, size), jnp.float32),
        in_specs=[HBM] * 9,
        out_specs=VMEM,
        scratch_shapes=[
            *buffers,
            pltpu.VMEM((share * n_mem + SUB, levels), jnp.float32),
            pltpu.VMEM((cols // LANE, pitch * channels, LANE), jnp.float32),
            pltpu.VMEM((channels, cols, levels), jnp.bfloat16),
            pltpu.VMEM((cols // GROUP * SUB, lanes), jnp.float32),
            pltpu.VMEM((cols // GROUP, height, lanes), jnp.bfloat16),
            pltpu.VMEM((blocks, lanes, capacity), jnp.bfloat16),
            pltpu.VMEM((blocks, height, capacity), jnp.bfloat16),
            pltpu.VMEM((blocks, n_mem, height, capacity), jnp.bfloat16),
            dma((9,)), dma((blocks, chips)), dma((blocks, chips)), dma((blocks, chips)), dma((blocks, chips)),
        ],
        compiler_params=pltpu.CompilerParams(
            collective_id=0, has_side_effects=True, vmem_limit_bytes=32 << 20
        ),
        name="gather",
    )(*args)
    dep_row = kinds * n_mem * height + 2 * GROUP
    dep_row -= (n_mem - kinds // share) * height - members - kinds % share
    total = size * n_mem
    gram, depart = pl.pallas_call(
        functools.partial(write_kernel, members, kinds, n_mem, height, dep_row),
        out_shape=(
            jax.ShapeDtypeStruct((1, size, total), jnp.float32),
            jax.ShapeDtypeStruct((1, size), jnp.float32),
        ),
        in_specs=[VMEM],
        out_specs=(HBM, HBM),
        scratch_shapes=[
            pltpu.VMEM((-(-size // LANE), total, LANE), jnp.float32),
            pltpu.VMEM((1, size, total), jnp.float32),
            pltpu.VMEM((1, size), jnp.float32),
            dma((1 + -(-total // LANE),)),
        ],
        compiler_params=pltpu.CompilerParams(vmem_limit_bytes=16 << 20),
        name="write",
    )(acc)
    return gram, depart


def solution(mesh):
    in_specs = (
        P("reg", "mem", None),
        P("reg", None, None),
        P("reg"),
        P("reg"),
        P("reg"),
        P(),
        P("reg", None, None),
        P("reg", None),
        P("reg", None, None),
    )
    out_specs = (P("reg", "mem", None), P("reg", "mem"))
    return jax.shard_map(local, mesh=mesh, in_specs=in_specs, out_specs=out_specs, check_vma=False)
```

```python
import functools

import jax
import jax.numpy as jnp
from jax import lax
from jax.experimental import pallas as pl
from jax.experimental.pallas import tpu as pltpu
from jax.sharding import PartitionSpec as P

ENS = 80
LANE = 128
SUB = 8
GROUP = 16
CROSS_REG = False
CROSS_HOP = True
LAG = 3
NT = (((1,), (1,)), ((), ()))
VMEM = pl.BlockSpec(memory_space=pltpu.VMEM)
HBM = pl.BlockSpec(memory_space=pltpu.MemorySpace.HBM)
MESH = pl.DeviceIdType.MESH


def iota(shape, dim):
    return lax.broadcasted_iota(jnp.int32, shape, dim)


def hot(mask):
    return jnp.where(mask, 1.0, 0.0).astype(jnp.bfloat16)


def times(left, right):
    return jnp.dot(left, right, preferred_element_type=jnp.float32)


def merge(a, b, bit, s, u):
    up = pltpu.roll(a, SUB - bit, 0)
    if b is None:
        return jnp.where((u & bit) != 0, up, a)
    low = (s & bit) == 0
    if 2 * bit == SUB:
        same = (s & bit) == (u & bit)
        return jnp.where(same, jnp.where(low, a, b), pltpu.roll(jnp.where(low, b, a), bit, 0))
    down = pltpu.roll(b, bit, 0)
    return jnp.where((u & bit) != 0, jnp.where(low, up, b), jnp.where(low, a, down))


def diagonal(parts, s, u):
    fours = [merge(parts[i], parts[i + 4] if len(parts) > 4 else None, 4, s, u) for i in range(4)]
    twos = [merge(fours[i], fours[i + 2], 2, s, u) for i in range(2)]
    return merge(twos[0], twos[1], 1, s, u)


def turn_jacobian(jac, wide, turned):
    levels, channels, cols = jac.shape
    pitch = wide.shape[1] // channels
    for l in range(levels):
        line = jac[l].astype(jnp.float32)
        for half in range(cols // LANE):
            for q in range(0, channels, SUB):
                part = line[q : q + SUB, half * LANE : (half + 1) * LANE]
                wide[half, pl.ds(q * pitch + l, SUB, stride=pitch), :] = part
    for half in range(cols // LANE):
        for q in range(channels):
            plane = wide[half, q * pitch : q * pitch + LANE, :]
            turned[q, half * LANE : (half + 1) * LANE, :] = plane.T[:, :levels].astype(jnp.bfloat16)


def side_rows(me, rinv, dep, level, modes, padded, extra, share):
    kinds, levels = modes.shape
    lanes = extra.shape[1]
    padded[...] = jnp.zeros_like(padded)
    padded[share : share + kinds, :] = modes[...] * ((ENS - 1) ** (-0.5))
    mine = padded[pl.ds(me * share, SUB), :].astype(jnp.bfloat16)
    s = iota((SUB, lanes), 0)
    holds_dep = (s == SUB - share + kinds % share) & (me == kinds // share)
    for g in range(extra.shape[0] // SUB):
        at = slice(g * lanes, (g + 1) * lanes)
        root = jnp.sqrt(rinv[:, at])
        high = root.astype(jnp.bfloat16).astype(jnp.float32)
        found = times(mine, hot(iota((levels, lanes), 0) == level[:, at]))
        found = jnp.where(holds_dep, dep[:, at] * root, found)
        found = jnp.where(s == 0, high, jnp.where(s == 1, root - high, found))
        extra[g * SUB : (g + 1) * SUB, :] = found
    channels = lanes // GROUP
    source, target = iota((lanes, lanes), 0), iota((lanes, lanes), 1)
    swap = hot(target == (source % channels) * GROUP + source // channels)
    extra[...] = times(extra[...].astype(jnp.bfloat16), swap)


def fill_table(prof, turned, extra, table):
    members, cols, levels = prof.shape
    groups, height, lanes = table.shape
    s, lane = iota((SUB, lanes), 0), iota((SUB, lanes), 1)
    u = lane % SUB
    upper = (lane // SUB) % 2 == 1

    def fill(g, carry):
        first = pl.ds(pl.multiple_of(g * GROUP, GROUP), GROUP)
        left = prof[:, first, :].reshape(members * GROUP, levels)
        right = turned[:, first, :].reshape(lanes, levels)
        full = lax.dot_general(left, right, NT, preferred_element_type=jnp.float32)
        parts = []
        for m in range(members):
            x = m * GROUP
            parts.append(jnp.where(upper, full[x + SUB : x + 2 * SUB], full[x : x + SUB]))
        more = extra[pl.ds(pl.multiple_of(g * SUB, SUB), SUB), :]
        root = more[0:1] + more[1:2]
        rows = [diagonal(parts[m : m + SUB], s, u) * root for m in range(0, members, SUB)]
        rows[-1] = jnp.where(s < members % SUB, rows[-1], more)
        table[g] = jnp.concatenate(rows, axis=0).astype(jnp.bfloat16)
        return carry

    lax.fori_loop(0, groups, fill, 0, unroll=16)


def gather_kernel(
    members, kinds, share, prof_h, jac_h, dep_h, rinv_h, level_h, modes_h, rows_h, counts_h, taper_h, acc,
    prof, jac, dep, rinv, level, modes, rows, counts, taper,
    padded, wide, turned, extra, table, picks, mine, region,
    s_in, s_reg, r_reg, s_hand, r_hand,
):
    blocks, height, capacity = mine.shape
    middle = blocks // 2
    n_mem, n_reg = lax.axis_size("mem"), lax.axis_size("reg")
    me, reg = lax.axis_index("mem"), lax.axis_index("reg")
    chips = n_mem // 2
    groups, _, lanes = table.shape
    channels = lanes // GROUP
    partner = {"mem": me + 1 - 2 * (me % 2), "reg": reg}
    pairs = [
        (level_h, level), (modes_h, modes), (rinv_h, rinv), (dep_h, dep), (rows_h, rows),
        (counts_h, counts), (taper_h, taper), (jac_h, jac), (prof_h, prof),
    ]
    loads = [pltpu.make_async_copy(h, v, s_in.at[i]) for i, (h, v) in enumerate(pairs)]
    for load in loads:
        load.start()

    def other(x):
        return x + 1 - 2 * lax.rem(x, 2)

    def target(d):
        to = lax.rem(reg + d - middle + n_reg, n_reg)
        return {"mem": other(me) if CROSS_REG else me, "reg": to}

    def peer(c):
        to = lax.rem(me + 2 * c, n_mem)
        return other(to) if CROSS_HOP else to

    def near(d, device):
        return jnp.where(d == middle, device, other(device)) if CROSS_REG else device

    def far(d, c):
        return near(d, peer(chips - c))

    def remote(src, dst, send, recv, device):
        return pltpu.make_async_remote_copy(
            src_ref=src, dst_ref=dst, send_sem=send, recv_sem=recv,
            device_id=device, device_id_type=MESH,
        )

    def across(d):
        return remote(mine.at[d], region.at[d, me], s_reg.at[d, 0], r_reg.at[d, 0], target(d))

    def hop(d, c):
        at = region.at[d, near(d, me)]
        to = {"mem": peer(c), "reg": reg}
        return remote(at, at, s_reg.at[d, c], r_reg.at[d, c], to)

    def hand(d, c):
        at = region.at[d, near(d, me) if c == 0 else far(d, c)]
        return remote(at, at, s_hand.at[d, c], r_hand.at[d, c], partner)

    def spread_out(d):
        for c in range(1, chips):
            hop(d, c).start()
        hand(d, 0).start()

    barrier = pltpu.get_barrier_semaphore()
    greeted = [target(d) for d in range(blocks) if d != middle]
    greeted += [partner] + [{"mem": peer(c), "reg": reg} for c in range(1, chips)]
    for device in greeted:
        pl.semaphore_signal(barrier, inc=1, device_id=device, device_id_type=MESH)

    at = lax.rem(middle - reg + n_reg, n_reg)
    lead = jnp.where(at < blocks, at, 0)

    def sent(k):
        return lax.rem(lead + k, blocks)

    def taken(k):
        return blocks - 1 - sent(k)

    for load in loads[:4]:
        load.wait()
    side_rows(me, rinv, dep, level, modes, padded, extra, share)
    for load in loads[4:7]:
        load.wait()

    def placed(d):
        live = iota((1, capacity), 1) < counts[0, d]
        return live, jnp.where(live, rows[d], 0)

    for d in range(blocks):
        _, picked = placed(d)
        low = (picked % channels) * GROUP + (picked // channels) % GROUP
        picks[d] = hot(iota((lanes, capacity), 0) == low)

    loads[7].wait()
    turn_jacobian(jac, wide, turned)
    loads[8].wait()
    fill_table(prof, turned, extra, table)

    s = iota((height, capacity), 0)
    is_dep = (s == members + kinds % share) & (me == kinds // share)
    for k in range(blocks):
        d = sent(k)
        live, picked = placed(d)
        high = picked // lanes
        found = times(table[...].reshape(groups * height, lanes), picks[d])
        chosen = found[:height]
        for h in range(1, groups):
            chosen = jnp.where(high == h, found[h * height : (h + 1) * height], chosen)
        root = jnp.sqrt(jnp.where(live, taper[d], 0.0))
        block = (chosen * jnp.where((s < members) | is_dep, root, 1.0)).astype(jnp.bfloat16)
        mine[d] = block
        if k == 0:
            pl.semaphore_wait(barrier, len(greeted))

        @pl.when(d == middle)
        def _():
            region[middle, me] = block
            spread_out(middle)

        @pl.when(d != middle)
        def _():
            across(d).start()

    acc[...] = jnp.zeros_like(acc)
    rows_of_eight = iota((SUB, capacity), 0)

    def joined(first, second, rolled=False):
        if not rolled:
            second = pltpu.roll(second, share, 0)
        seam = jnp.where(rows_of_eight < SUB - share, first[height - SUB :], second[:SUB])
        return jnp.concatenate([first[: height - SUB], seam, second[SUB:]], axis=0)

    def forward(k):
        d = taken(k)

        @pl.when(d != middle)
        def _():
            across(d).wait_recv()
            spread_out(d)

    def pass_on(k):
        d = taken(k)
        for c in range(1, chips):
            hop(d, c).wait_recv()
            hand(d, c).start()

    def multiply(k):
        d = taken(k)
        for c in range(chips):
            hand(d, c).wait_recv()
        parts = [region[d, j].astype(jnp.float32) for j in range(n_mem)]
        every = [joined(parts[j], parts[j + 1]) for j in range(0, n_mem, 2)]
        every = jnp.concatenate(every, axis=0).astype(jnp.bfloat16)
        low = region[d, me].astype(jnp.float32)
        high = pltpu.roll(low, share, 0)
        lines = []
        for l in range(kinds):
            at = members + l % share
            lines.append(parts[l // share][at : at + 1])
        own = []
        for l in range(0, kinds, 2):
            own.append(joined(low * lines[l], high * lines[l + 1], True))
        own = jnp.concatenate(own, axis=0).astype(jnp.bfloat16)
        left = []
        for line in lines:
            tall = jnp.broadcast_to(line, (GROUP, capacity)).astype(jnp.bfloat16)
            left.append(every * jnp.concatenate([tall] * (every.shape[0] // GROUP), axis=0))
        last = parts[kinds // share][height - SUB :]
        left.append(jnp.concatenate([last, last], axis=0).astype(jnp.bfloat16))
        left = jnp.concatenate(left, axis=0)
        acc[...] += lax.dot_general(left, own, NT, preferred_element_type=jnp.float32)

    def step(k, carry):
        @pl.when(k < blocks)
        def _():
            forward(k)

        @pl.when((k >= LAG) & (k < blocks + LAG))
        def _():
            pass_on(k - LAG)

        @pl.when(k > LAG)
        def _():
            multiply(k - LAG - 1)

        return carry

    lax.fori_loop(0, blocks + LAG + 1, step, 0)
    for d in range(blocks):
        if d != middle:
            across(d).wait_send()
        for c in range(1, chips):
            hop(d, c).wait_send()
        for c in range(chips):
            hand(d, c).wait_send()


def write_kernel(members, kinds, n_mem, dep_row, acc, gram, depart, rows, lines, out, out_dep, sems):
    size = members * kinds
    total = size * n_mem
    every = members * n_mem
    tiles = -(-size // LANE)
    for t in range(tiles):
        wide = min(LANE, size - t * LANE)
        for l in range(kinds):
            part = acc[l * every : (l + 1) * every, t * LANE : t * LANE + wide]
            rows[t, pl.ds(l, every, stride=kinds), 0:wide] = part
    row, col = iota((size, size), 0), iota((size, size), 1)
    swap = jnp.where(col == (row % members) * kinds + row // members, 1.0, 0.0)
    out_dep[...] = jnp.dot(
        acc[dep_row : dep_row + 1, :], swap, precision=lax.Precision.HIGHEST,
        preferred_element_type=jnp.float32,
    )
    copies = [pltpu.make_async_copy(out_dep, depart, sems.at[0])]
    copies[0].start()
    for i in range(-(-total // LANE)):
        at = slice(i * LANE, min(total, (i + 1) * LANE))
        tall = at.stop - at.start
        turned = [rows[t, at, :].T[: min(LANE, size - t * LANE)] for t in range(tiles)]
        turned = jnp.concatenate(turned, axis=0)
        for k in range(kinds):
            part = turned[k * members : (k + 1) * members]
            lines[i, pl.ds(k, members, stride=kinds), 0:tall] = part
        out[0, :, at] = lines[i, :, 0:tall]
        copy = pltpu.make_async_copy(out.at[:, :, at], gram.at[:, :, at], sems.at[1 + i])
        copy.start()
        copies.append(copy)
    for copy in copies:
        copy.wait()


def local(
    profiles, jacobian, departure, obs_rinv, obs_level, vertical_modes, send_rows, counts, loc_taper
):
    cols, members, levels = profiles.shape
    channels = jacobian.shape[1]
    blocks, capacity = send_rows.shape[1], send_rows.shape[2]
    kinds = vertical_modes.shape[1]
    n_mem = lax.axis_size("mem")
    chips = n_mem // 2
    share = -(-(kinds + 1) // n_mem)
    height = members + share
    size = members * kinds
    lanes = GROUP * channels
    dma = pltpu.SemaphoreType.DMA
    args = (
        profiles.transpose(1, 0, 2), jacobian.transpose(2, 1, 0),
        departure[None], obs_rinv[None], obs_level[None], vertical_modes.T,
        send_rows.transpose(1, 0, 2), counts, loc_taper.transpose(1, 0, 2),
    )
    args = [pltpu.with_memory_space_constraint(a, pltpu.MemorySpace.HBM) for a in args]
    buffers = [pltpu.VMEM(a.shape, a.dtype) for a in args]
    buffers[7] = pltpu.SMEM(counts.shape, counts.dtype)
    pitch = -(-levels // LANE) * LANE + 1
    acc_rows = size * n_mem + GROUP
    acc = pl.pallas_call(
        functools.partial(gather_kernel, members, kinds, share),
        out_shape=jax.ShapeDtypeStruct((acc_rows, size), jnp.float32),
        in_specs=[HBM] * 9,
        out_specs=VMEM,
        scratch_shapes=[
            *buffers,
            pltpu.VMEM((share * n_mem + SUB, levels), jnp.float32),
            pltpu.VMEM((cols // LANE, pitch * channels, LANE), jnp.float32),
            pltpu.VMEM((channels, cols, levels), jnp.bfloat16),
            pltpu.VMEM((cols // GROUP * SUB, lanes), jnp.float32),
            pltpu.VMEM((cols // GROUP, height, lanes), jnp.bfloat16),
            pltpu.VMEM((blocks, lanes, capacity), jnp.bfloat16),
            pltpu.VMEM((blocks, height, capacity), jnp.bfloat16),
            pltpu.VMEM((blocks, n_mem, height, capacity), jnp.bfloat16),
            dma((9,)), dma((blocks, chips)), dma((blocks, chips)), dma((blocks, chips)), dma((blocks, chips)),
        ],
        compiler_params=pltpu.CompilerParams(
            collective_id=0, has_side_effects=True, vmem_limit_bytes=32 << 20
        ),
        name="gather",
    )(*args)
    dep_row = size * n_mem + SUB - share + kinds % share
    total = size * n_mem
    gram, depart = pl.pallas_call(
        functools.partial(write_kernel, members, kinds, n_mem, dep_row),
        out_shape=(
            jax.ShapeDtypeStruct((1, size, total), jnp.float32),
            jax.ShapeDtypeStruct((1, size), jnp.float32),
        ),
        in_specs=[VMEM],
        out_specs=(HBM, HBM),
        scratch_shapes=[
            pltpu.VMEM((-(-size // LANE), total, LANE), jnp.float32),
            pltpu.VMEM((-(-total // LANE), size, LANE), jnp.float32),
            pltpu.VMEM((1, size, total), jnp.float32),
            pltpu.VMEM((1, size), jnp.float32),
            dma((1 + -(-total // LANE),)),
        ],
        compiler_params=pltpu.CompilerParams(vmem_limit_bytes=16 << 20),
        name="write",
    )(acc)
    return gram, depart


def solution(mesh):
    in_specs = (
        P("reg", "mem", None),
        P("reg", None, None),
        P("reg"),
        P("reg"),
        P("reg"),
        P(),
        P("reg", None, None),
        P("reg", None),
        P("reg", None, None),
    )
    out_specs = (P("reg", "mem", None), P("reg", "mem"))
    return jax.shard_map(local, mesh=mesh, in_specs=in_specs, out_specs=out_specs, check_vma=False)
```

```python
import functools

import jax
import jax.numpy as jnp
from jax import lax
from jax.experimental import pallas as pl
from jax.experimental.pallas import tpu as pltpu
from jax.sharding import PartitionSpec as P

ENS = 80
LANE = 128
SUB = 8
GROUP = 16
CROSS_REG = False
CROSS_HOP = True
LAG = 4
NT = (((1,), (1,)), ((), ()))
VMEM = pl.BlockSpec(memory_space=pltpu.VMEM)
HBM = pl.BlockSpec(memory_space=pltpu.MemorySpace.HBM)
MESH = pl.DeviceIdType.MESH


def iota(shape, dim):
    return lax.broadcasted_iota(jnp.int32, shape, dim)


def hot(mask):
    return jnp.where(mask, 1.0, 0.0).astype(jnp.bfloat16)


def times(left, right):
    return jnp.dot(left, right, preferred_element_type=jnp.float32)


def merge(a, b, bit, s, u):
    up = pltpu.roll(a, SUB - bit, 0)
    if b is None:
        return jnp.where((u & bit) != 0, up, a)
    low = (s & bit) == 0
    if 2 * bit == SUB:
        same = (s & bit) == (u & bit)
        return jnp.where(same, jnp.where(low, a, b), pltpu.roll(jnp.where(low, b, a), bit, 0))
    down = pltpu.roll(b, bit, 0)
    return jnp.where((u & bit) != 0, jnp.where(low, up, b), jnp.where(low, a, down))


def diagonal(parts, s, u):
    fours = [merge(parts[i], parts[i + 4] if len(parts) > 4 else None, 4, s, u) for i in range(4)]
    twos = [merge(fours[i], fours[i + 2], 2, s, u) for i in range(2)]
    return merge(twos[0], twos[1], 1, s, u)


def turn_jacobian(jac, wide, turned):
    levels, channels, cols = jac.shape
    pitch = wide.shape[1] // channels
    for l in range(levels):
        line = jac[l].astype(jnp.float32)
        for half in range(cols // LANE):
            for q in range(0, channels, SUB):
                part = line[q : q + SUB, half * LANE : (half + 1) * LANE]
                wide[half, pl.ds(q * pitch + l, SUB, stride=pitch), :] = part
    for half in range(cols // LANE):
        for q in range(channels):
            plane = wide[half, q * pitch : q * pitch + LANE, :]
            turned[q, half * LANE : (half + 1) * LANE, :] = plane.T[:, :levels].astype(jnp.bfloat16)


def side_rows(me, rinv, dep, level, modes, padded, extra, share):
    kinds, levels = modes.shape
    lanes = extra.shape[1]
    padded[...] = jnp.zeros_like(padded)
    padded[share : share + kinds, :] = modes[...] * ((ENS - 1) ** (-0.5))
    mine = padded[pl.ds(me * share, SUB), :].astype(jnp.bfloat16)
    s = iota((SUB, lanes), 0)
    holds_dep = (s == SUB - share + kinds % share) & (me == kinds // share)
    for g in range(extra.shape[0] // SUB):
        at = slice(g * lanes, (g + 1) * lanes)
        root = jnp.sqrt(rinv[:, at])
        high = root.astype(jnp.bfloat16).astype(jnp.float32)
        found = times(mine, hot(iota((levels, lanes), 0) == level[:, at]))
        found = jnp.where(holds_dep, dep[:, at] * root, found)
        found = jnp.where(s == 0, high, jnp.where(s == 1, root - high, found))
        extra[g * SUB : (g + 1) * SUB, :] = found
    channels = lanes // GROUP
    source, target = iota((lanes, lanes), 0), iota((lanes, lanes), 1)
    swap = hot(target == (source % channels) * GROUP + source // channels)
    extra[...] = times(extra[...].astype(jnp.bfloat16), swap)


def fill_table(prof, turned, extra, table):
    members, cols, levels = prof.shape
    groups, height, lanes = table.shape
    s, lane = iota((SUB, lanes), 0), iota((SUB, lanes), 1)
    u = lane % SUB
    upper = (lane // SUB) % 2 == 1

    def fill(g, carry):
        first = pl.ds(pl.multiple_of(g * GROUP, GROUP), GROUP)
        left = prof[:, first, :].reshape(members * GROUP, levels)
        right = turned[:, first, :].reshape(lanes, levels)
        full = lax.dot_general(left, right, NT, preferred_element_type=jnp.float32)
        parts = []
        for m in range(members):
            x = m * GROUP
            parts.append(jnp.where(upper, full[x + SUB : x + 2 * SUB], full[x : x + SUB]))
        more = extra[pl.ds(pl.multiple_of(g * SUB, SUB), SUB), :]
        root = more[0:1] + more[1:2]
        rows = [diagonal(parts[m : m + SUB], s, u) * root for m in range(0, members, SUB)]
        rows[-1] = jnp.where(s < members % SUB, rows[-1], more)
        table[g] = jnp.concatenate(rows, axis=0).astype(jnp.bfloat16)
        return carry

    lax.fori_loop(0, groups, fill, 0, unroll=16)


def gather_kernel(
    members, kinds, share, prof_h, jac_h, dep_h, rinv_h, level_h, modes_h, rows_h, counts_h, taper_h, acc,
    prof, jac, dep, rinv, level, modes, rows, counts, taper,
    padded, wide, turned, extra, table, picks, mine, region,
    s_in, s_reg, r_reg, s_hand, r_hand,
):
    blocks, height, capacity = mine.shape
    middle = blocks // 2
    n_mem, n_reg = lax.axis_size("mem"), lax.axis_size("reg")
    me, reg = lax.axis_index("mem"), lax.axis_index("reg")
    chips = n_mem // 2
    groups, _, lanes = table.shape
    channels = lanes // GROUP
    partner = {"mem": me + 1 - 2 * (me % 2), "reg": reg}
    pairs = [
        (level_h, level), (modes_h, modes), (rinv_h, rinv), (dep_h, dep), (rows_h, rows),
        (counts_h, counts), (taper_h, taper), (jac_h, jac), (prof_h, prof),
    ]
    loads = [pltpu.make_async_copy(h, v, s_in.at[i]) for i, (h, v) in enumerate(pairs)]
    for load in loads:
        load.start()

    def other(x):
        return x + 1 - 2 * lax.rem(x, 2)

    def target(d):
        to = lax.rem(reg + d - middle + n_reg, n_reg)
        return {"mem": other(me) if CROSS_REG else me, "reg": to}

    def peer(c):
        to = lax.rem(me + 2 * c, n_mem)
        return other(to) if CROSS_HOP else to

    def near(d, device):
        return jnp.where(d == middle, device, other(device)) if CROSS_REG else device

    def far(d, c):
        return near(d, peer(chips - c))

    def remote(src, dst, send, recv, device):
        return pltpu.make_async_remote_copy(
            src_ref=src, dst_ref=dst, send_sem=send, recv_sem=recv,
            device_id=device, device_id_type=MESH,
        )

    def across(d):
        return remote(mine.at[d], region.at[d, me], s_reg.at[d, 0], r_reg.at[d, 0], target(d))

    def hop(d, c):
        at = region.at[d, near(d, me)]
        to = {"mem": peer(c), "reg": reg}
        return remote(at, at, s_reg.at[d, c], r_reg.at[d, c], to)

    def hand(d, c):
        at = region.at[d, near(d, me) if c == 0 else far(d, c)]
        return remote(at, at, s_hand.at[d, c], r_hand.at[d, c], partner)

    def spread_out(d):
        for c in range(1, chips):
            hop(d, c).start()
        hand(d, 0).start()

    barrier = pltpu.get_barrier_semaphore()
    greeted = [target(d) for d in range(blocks) if d != middle]
    greeted += [partner] + [{"mem": peer(c), "reg": reg} for c in range(1, chips)]
    for device in greeted:
        pl.semaphore_signal(barrier, inc=1, device_id=device, device_id_type=MESH)

    at = lax.rem(middle - reg + n_reg, n_reg)
    lead = jnp.where(at < blocks, at, 0)

    def sent(k):
        return lax.rem(lead + k, blocks)

    def taken(k):
        return blocks - 1 - sent(k)

    for load in loads[:4]:
        load.wait()
    side_rows(me, rinv, dep, level, modes, padded, extra, share)
    for load in loads[4:7]:
        load.wait()

    def placed(d):
        live = iota((1, capacity), 1) < counts[0, d]
        return live, jnp.where(live, rows[d], 0)

    for d in range(blocks):
        _, picked = placed(d)
        low = (picked % channels) * GROUP + (picked // channels) % GROUP
        picks[d] = hot(iota((lanes, capacity), 0) == low)

    loads[7].wait()
    turn_jacobian(jac, wide, turned)
    loads[8].wait()
    fill_table(prof, turned, extra, table)

    s = iota((height, capacity), 0)
    is_dep = (s == members + kinds % share) & (me == kinds // share)
    for k in range(blocks):
        d = sent(k)
        live, picked = placed(d)
        high = picked // lanes
        found = times(table[...].reshape(groups * height, lanes), picks[d])
        chosen = found[:height]
        for h in range(1, groups):
            chosen = jnp.where(high == h, found[h * height : (h + 1) * height], chosen)
        root = jnp.sqrt(jnp.where(live, taper[d], 0.0))
        block = (chosen * jnp.where((s < members) | is_dep, root, 1.0)).astype(jnp.bfloat16)
        mine[d] = block
        if k == 0:
            pl.semaphore_wait(barrier, len(greeted))

        @pl.when(d == middle)
        def _():
            region[middle, me] = block
            spread_out(middle)

        @pl.when(d != middle)
        def _():
            across(d).start()

    acc[...] = jnp.zeros_like(acc)
    rows_of_eight = iota((SUB, capacity), 0)

    def joined(first, second, rolled=False):
        if not rolled:
            second = pltpu.roll(second, share, 0)
        seam = jnp.where(rows_of_eight < SUB - share, first[height - SUB :], second[:SUB])
        return jnp.concatenate([first[: height - SUB], seam, second[SUB:]], axis=0)

    def forward(k):
        d = taken(k)

        @pl.when(d != middle)
        def _():
            across(d).wait_recv()
            spread_out(d)

    def pass_on(k):
        d = taken(k)
        for c in range(1, chips):
            hop(d, c).wait_recv()
            hand(d, c).start()

    def multiply(k):
        d = taken(k)
        for c in range(chips):
            hand(d, c).wait_recv()
        parts = [region[d, j].astype(jnp.float32) for j in range(n_mem)]
        every = [joined(parts[j], parts[j + 1]) for j in range(0, n_mem, 2)]
        every = jnp.concatenate(every, axis=0).astype(jnp.bfloat16)
        low = region[d, me].astype(jnp.float32)
        high = pltpu.roll(low, share, 0)
        lines = []
        for l in range(kinds):
            at = members + l % share
            lines.append(parts[l // share][at : at + 1])
        own = []
        for l in range(0, kinds, 2):
            own.append(joined(low * lines[l], high * lines[l + 1], True))
        own = jnp.concatenate(own, axis=0).astype(jnp.bfloat16)
        left = []
        for line in lines:
            tall = jnp.broadcast_to(line, (GROUP, capacity)).astype(jnp.bfloat16)
            left.append(every * jnp.concatenate([tall] * (every.shape[0] // GROUP), axis=0))
        last = parts[kinds // share][height - SUB :]
        left.append(jnp.concatenate([last, last], axis=0).astype(jnp.bfloat16))
        left = jnp.concatenate(left, axis=0)
        acc[...] += lax.dot_general(left, own, NT, preferred_element_type=jnp.float32)

    def step(k, carry):
        @pl.when(k < blocks)
        def _():
            forward(k)

        @pl.when((k >= LAG) & (k < blocks + LAG))
        def _():
            pass_on(k - LAG)

        @pl.when(k >= LAG + 2)
        def _():
            multiply(k - LAG - 2)

        return carry

    lax.fori_loop(0, blocks + LAG + 2, step, 0)
    for d in range(blocks):
        if d != middle:
            across(d).wait_send()
        for c in range(1, chips):
            hop(d, c).wait_send()
        for c in range(chips):
            hand(d, c).wait_send()


def write_kernel(members, kinds, n_mem, dep_row, acc, gram, depart, rows, lines, out, out_dep, sems):
    size = members * kinds
    total = size * n_mem
    every = members * n_mem
    tiles = -(-size // LANE)
    for t in range(tiles):
        wide = min(LANE, size - t * LANE)
        for l in range(kinds):
            part = acc[l * every : (l + 1) * every, t * LANE : t * LANE + wide]
            rows[t, pl.ds(l, every, stride=kinds), 0:wide] = part
    row, col = iota((size, size), 0), iota((size, size), 1)
    swap = jnp.where(col == (row % members) * kinds + row // members, 1.0, 0.0)
    out_dep[...] = jnp.dot(
        acc[dep_row : dep_row + 1, :], swap, precision=lax.Precision.HIGHEST,
        preferred_element_type=jnp.float32,
    )
    copies = [pltpu.make_async_copy(out_dep, depart, sems.at[0])]
    copies[0].start()
    for i in range(-(-total // LANE)):
        at = slice(i * LANE, min(total, (i + 1) * LANE))
        tall = at.stop - at.start
        turned = [rows[t, at, :].T[: min(LANE, size - t * LANE)] for t in range(tiles)]
        turned = jnp.concatenate(turned, axis=0)
        for k in range(kinds):
            part = turned[k * members : (k + 1) * members]
            lines[i, pl.ds(k, members, stride=kinds), 0:tall] = part
        out[0, :, at] = lines[i, :, 0:tall]
        copy = pltpu.make_async_copy(out.at[:, :, at], gram.at[:, :, at], sems.at[1 + i])
        copy.start()
        copies.append(copy)
    for copy in copies:
        copy.wait()


def local(
    profiles, jacobian, departure, obs_rinv, obs_level, vertical_modes, send_rows, counts, loc_taper
):
    cols, members, levels = profiles.shape
    channels = jacobian.shape[1]
    blocks, capacity = send_rows.shape[1], send_rows.shape[2]
    kinds = vertical_modes.shape[1]
    n_mem = lax.axis_size("mem")
    chips = n_mem // 2
    share = -(-(kinds + 1) // n_mem)
    height = members + share
    size = members * kinds
    lanes = GROUP * channels
    dma = pltpu.SemaphoreType.DMA
    args = (
        profiles.transpose(1, 0, 2), jacobian.transpose(2, 1, 0),
        departure[None], obs_rinv[None], obs_level[None], vertical_modes.T,
        send_rows.transpose(1, 0, 2), counts, loc_taper.transpose(1, 0, 2),
    )
    args = [pltpu.with_memory_space_constraint(a, pltpu.MemorySpace.HBM) for a in args]
    buffers = [pltpu.VMEM(a.shape, a.dtype) for a in args]
    buffers[7] = pltpu.SMEM(counts.shape, counts.dtype)
    pitch = -(-levels // LANE) * LANE + 1
    acc_rows = size * n_mem + GROUP
    acc = pl.pallas_call(
        functools.partial(gather_kernel, members, kinds, share),
        out_shape=jax.ShapeDtypeStruct((acc_rows, size), jnp.float32),
        in_specs=[HBM] * 9,
        out_specs=VMEM,
        scratch_shapes=[
            *buffers,
            pltpu.VMEM((share * n_mem + SUB, levels), jnp.float32),
            pltpu.VMEM((cols // LANE, pitch * channels, LANE), jnp.float32),
            pltpu.VMEM((channels, cols, levels), jnp.bfloat16),
            pltpu.VMEM((cols // GROUP * SUB, lanes), jnp.float32),
            pltpu.VMEM((cols // GROUP, height, lanes), jnp.bfloat16),
            pltpu.VMEM((blocks, lanes, capacity), jnp.bfloat16),
            pltpu.VMEM((blocks, height, capacity), jnp.bfloat16),
            pltpu.VMEM((blocks, n_mem, height, capacity), jnp.bfloat16),
            dma((9,)), dma((blocks, chips)), dma((blocks, chips)), dma((blocks, chips)), dma((blocks, chips)),
        ],
        compiler_params=pltpu.CompilerParams(
            collective_id=0, has_side_effects=True, vmem_limit_bytes=32 << 20
        ),
        name="gather",
    )(*args)
    dep_row = size * n_mem + SUB - share + kinds % share
    total = size * n_mem
    gram, depart = pl.pallas_call(
        functools.partial(write_kernel, members, kinds, n_mem, dep_row),
        out_shape=(
            jax.ShapeDtypeStruct((1, size, total), jnp.float32),
            jax.ShapeDtypeStruct((1, size), jnp.float32),
        ),
        in_specs=[VMEM],
        out_specs=(HBM, HBM),
        scratch_shapes=[
            pltpu.VMEM((-(-size // LANE), total, LANE), jnp.float32),
            pltpu.VMEM((-(-total // LANE), size, LANE), jnp.float32),
            pltpu.VMEM((1, size, total), jnp.float32),
            pltpu.VMEM((1, size), jnp.float32),
            dma((1 + -(-total // LANE),)),
        ],
        compiler_params=pltpu.CompilerParams(vmem_limit_bytes=16 << 20),
        name="write",
    )(acc)
    return gram, depart


def solution(mesh):
    in_specs = (
        P("reg", "mem", None),
        P("reg", None, None),
        P("reg"),
        P("reg"),
        P("reg"),
        P(),
        P("reg", None, None),
        P("reg", None),
        P("reg", None, None),
    )
    out_specs = (P("reg", "mem", None), P("reg", "mem"))
    return jax.shard_map(local, mesh=mesh, in_specs=in_specs, out_specs=out_specs, check_vma=False)
```

```python
import functools

import jax
import jax.numpy as jnp
from jax import lax
from jax.experimental import pallas as pl
from jax.experimental.pallas import tpu as pltpu
from jax.sharding import PartitionSpec as P

ENS = 80
LANE = 128
SUB = 8
GROUP = 16
CROSS_REG = False
CROSS_HOP = True
LAG = 4
NT = (((1,), (1,)), ((), ()))
VMEM = pl.BlockSpec(memory_space=pltpu.VMEM)
HBM = pl.BlockSpec(memory_space=pltpu.MemorySpace.HBM)
MESH = pl.DeviceIdType.MESH


def iota(shape, dim):
    return lax.broadcasted_iota(jnp.int32, shape, dim)


def hot(mask):
    return jnp.where(mask, 1.0, 0.0).astype(jnp.bfloat16)


def times(left, right):
    return jnp.dot(left, right, preferred_element_type=jnp.float32)


def merge(a, b, bit, s, u):
    up = pltpu.roll(a, SUB - bit, 0)
    if b is None:
        return jnp.where((u & bit) != 0, up, a)
    low = (s & bit) == 0
    if 2 * bit == SUB:
        same = (s & bit) == (u & bit)
        return jnp.where(same, jnp.where(low, a, b), pltpu.roll(jnp.where(low, b, a), bit, 0))
    down = pltpu.roll(b, bit, 0)
    return jnp.where((u & bit) != 0, jnp.where(low, up, b), jnp.where(low, a, down))


def diagonal(parts, s, u):
    fours = [merge(parts[i], parts[i + 4] if len(parts) > 4 else None, 4, s, u) for i in range(4)]
    twos = [merge(fours[i], fours[i + 2], 2, s, u) for i in range(2)]
    return merge(twos[0], twos[1], 1, s, u)


def turn_jacobian(jac, wide, turned):
    levels, channels, cols = jac.shape
    pitch = wide.shape[1] // channels
    for l in range(levels):
        line = jac[l].astype(jnp.float32)
        for half in range(cols // LANE):
            for q in range(0, channels, SUB):
                part = line[q : q + SUB, half * LANE : (half + 1) * LANE]
                wide[half, pl.ds(q * pitch + l, SUB, stride=pitch), :] = part
    for half in range(cols // LANE):
        for q in range(channels):
            plane = wide[half, q * pitch : q * pitch + LANE, :]
            turned[q, half * LANE : (half + 1) * LANE, :] = plane.T[:, :levels].astype(jnp.bfloat16)


def side_rows(me, rinv, dep, level, modes, padded, extra, share):
    kinds, levels = modes.shape
    lanes = extra.shape[1]
    padded[...] = jnp.zeros_like(padded)
    padded[share : share + kinds, :] = modes[...] * ((ENS - 1) ** (-0.5))
    mine = padded[pl.ds(me * share, SUB), :].astype(jnp.bfloat16)
    s = iota((SUB, lanes), 0)
    holds_dep = (s == SUB - share + kinds % share) & (me == kinds // share)
    for g in range(extra.shape[0] // SUB):
        at = slice(g * lanes, (g + 1) * lanes)
        root = jnp.sqrt(rinv[:, at])
        high = root.astype(jnp.bfloat16).astype(jnp.float32)
        found = times(mine, hot(iota((levels, lanes), 0) == level[:, at]))
        found = jnp.where(holds_dep, dep[:, at] * root, found)
        found = jnp.where(s == 0, high, jnp.where(s == 1, root - high, found))
        extra[g * SUB : (g + 1) * SUB, :] = found
    channels = lanes // GROUP
    source, target = iota((lanes, lanes), 0), iota((lanes, lanes), 1)
    swap = hot(target == (source % channels) * GROUP + source // channels)
    extra[...] = times(extra[...].astype(jnp.bfloat16), swap)


def fill_table(prof, turned, extra, table):
    members, cols, levels = prof.shape
    groups, height, lanes = table.shape
    s, lane = iota((SUB, lanes), 0), iota((SUB, lanes), 1)
    u = lane % SUB
    upper = (lane // SUB) % 2 == 1

    def fill(g, carry):
        first = pl.ds(pl.multiple_of(g * GROUP, GROUP), GROUP)
        left = prof[:, first, :].reshape(members * GROUP, levels)
        right = turned[:, first, :].reshape(lanes, levels)
        full = lax.dot_general(left, right, NT, preferred_element_type=jnp.float32)
        parts = []
        for m in range(members):
            x = m * GROUP
            parts.append(jnp.where(upper, full[x + SUB : x + 2 * SUB], full[x : x + SUB]))
        more = extra[pl.ds(pl.multiple_of(g * SUB, SUB), SUB), :]
        root = more[0:1] + more[1:2]
        rows = [diagonal(parts[m : m + SUB], s, u) * root for m in range(0, members, SUB)]
        rows[-1] = jnp.where(s < members % SUB, rows[-1], more)
        table[g] = jnp.concatenate(rows, axis=0).astype(jnp.bfloat16)
        return carry

    lax.fori_loop(0, groups, fill, 0, unroll=16)


def gather_kernel(
    members, kinds, share, prof_h, jac_h, dep_h, rinv_h, level_h, modes_h, rows_h, counts_h, taper_h, acc,
    prof, jac, dep, rinv, level, modes, rows, counts, taper,
    padded, wide, turned, extra, table, mine, region,
    s_in, s_reg, r_reg, s_hand, r_hand,
):
    blocks, height, capacity = mine.shape
    middle = blocks // 2
    n_mem, n_reg = lax.axis_size("mem"), lax.axis_size("reg")
    me, reg = lax.axis_index("mem"), lax.axis_index("reg")
    chips = n_mem // 2
    groups, _, lanes = table.shape
    channels = lanes // GROUP
    partner = {"mem": me + 1 - 2 * (me % 2), "reg": reg}
    pairs = [
        (level_h, level), (modes_h, modes), (rinv_h, rinv), (dep_h, dep), (rows_h, rows),
        (counts_h, counts), (taper_h, taper), (jac_h, jac), (prof_h, prof),
    ]
    loads = [pltpu.make_async_copy(h, v, s_in.at[i]) for i, (h, v) in enumerate(pairs)]
    for load in loads:
        load.start()

    def other(x):
        return x + 1 - 2 * lax.rem(x, 2)

    def target(d):
        to = lax.rem(reg + d - middle + n_reg, n_reg)
        return {"mem": other(me) if CROSS_REG else me, "reg": to}

    def peer(c):
        to = lax.rem(me + 2 * c, n_mem)
        return other(to) if CROSS_HOP else to

    def near(d, device):
        return jnp.where(d == middle, device, other(device)) if CROSS_REG else device

    def far(d, c):
        return near(d, peer(chips - c))

    def remote(src, dst, send, recv, device):
        return pltpu.make_async_remote_copy(
            src_ref=src, dst_ref=dst, send_sem=send, recv_sem=recv,
            device_id=device, device_id_type=MESH,
        )

    def across(d):
        return remote(mine.at[d], region.at[d, me], s_reg.at[d, 0], r_reg.at[d, 0], target(d))

    def hop(d, c):
        at = region.at[d, near(d, me)]
        to = {"mem": peer(c), "reg": reg}
        return remote(at, at, s_reg.at[d, c], r_reg.at[d, c], to)

    def hand(d, c):
        at = region.at[d, near(d, me) if c == 0 else far(d, c)]
        return remote(at, at, s_hand.at[d, c], r_hand.at[d, c], partner)

    def spread_out(d):
        for c in range(1, chips):
            hop(d, c).start()
        hand(d, 0).start()

    barrier = pltpu.get_barrier_semaphore()
    greeted = [target(d) for d in range(blocks) if d != middle]
    greeted += [partner] + [{"mem": peer(c), "reg": reg} for c in range(1, chips)]
    for device in greeted:
        pl.semaphore_signal(barrier, inc=1, device_id=device, device_id_type=MESH)

    at = lax.rem(middle - reg + n_reg, n_reg)
    lead = jnp.where(at < blocks, at, 0)

    def sent(k):
        return lax.rem(lead + k, blocks)

    late = 4 * reg >= 3 * n_reg

    def taken(k):
        return blocks - 1 - lax.rem(lead + jnp.where(late, blocks - 1 - k, k), blocks)

    for load in loads[:4]:
        load.wait()
    side_rows(me, rinv, dep, level, modes, padded, extra, share)
    for load in loads[4:7]:
        load.wait()

    def placed(d):
        live = iota((1, capacity), 1) < counts[0, d]
        return live, jnp.where(live, rows[d], 0)

    loads[7].wait()
    turn_jacobian(jac, wide, turned)
    loads[8].wait()
    fill_table(prof, turned, extra, table)

    s = iota((height, capacity), 0)
    is_dep = (s == members + kinds % share) & (me == kinds // share)
    for k in range(blocks):
        d = sent(k)
        live, picked = placed(d)
        high = picked // lanes
        low = (picked % channels) * GROUP + (picked // channels) % GROUP
        found = times(table[...].reshape(groups * height, lanes), hot(iota((lanes, capacity), 0) == low))
        chosen = found[:height]
        for h in range(1, groups):
            chosen = jnp.where(high == h, found[h * height : (h + 1) * height], chosen)
        root = jnp.sqrt(jnp.where(live, taper[d], 0.0))
        block = (chosen * jnp.where((s < members) | is_dep, root, 1.0)).astype(jnp.bfloat16)
        mine[d] = block
        if k == 0:
            pl.semaphore_wait(barrier, len(greeted))

        @pl.when(d == middle)
        def _():
            region[middle, me] = block
            spread_out(middle)

        @pl.when(d != middle)
        def _():
            across(d).start()

    acc[...] = jnp.zeros_like(acc)
    rows_of_eight = iota((SUB, capacity), 0)

    def joined(first, second, rolled=False):
        if not rolled:
            second = pltpu.roll(second, share, 0)
        seam = jnp.where(rows_of_eight < SUB - share, first[height - SUB :], second[:SUB])
        return jnp.concatenate([first[: height - SUB], seam, second[SUB:]], axis=0)

    def forward(k):
        d = taken(k)

        @pl.when(d != middle)
        def _():
            across(d).wait_recv()
            spread_out(d)

    def pass_on(k):
        d = taken(k)
        for c in range(1, chips):
            hop(d, c).wait_recv()
            hand(d, c).start()

    def multiply(k):
        d = taken(k)
        for c in range(chips):
            hand(d, c).wait_recv()
        parts = [region[d, j].astype(jnp.float32) for j in range(n_mem)]
        every = [joined(parts[j], parts[j + 1]) for j in range(0, n_mem, 2)]
        every = jnp.concatenate(every, axis=0).astype(jnp.bfloat16)
        low = region[d, me].astype(jnp.float32)
        high = pltpu.roll(low, share, 0)
        lines = []
        for l in range(kinds):
            at = members + l % share
            lines.append(parts[l // share][at : at + 1])
        own = []
        for l in range(0, kinds, 2):
            own.append(joined(low * lines[l], high * lines[l + 1], True))
        own = jnp.concatenate(own, axis=0).astype(jnp.bfloat16)
        left = []
        for line in lines:
            tall = jnp.broadcast_to(line, (GROUP, capacity)).astype(jnp.bfloat16)
            left.append(every * jnp.concatenate([tall] * (every.shape[0] // GROUP), axis=0))
        last = parts[kinds // share][height - SUB :]
        left.append(jnp.concatenate([last, last], axis=0).astype(jnp.bfloat16))
        left = jnp.concatenate(left, axis=0)
        acc[...] += lax.dot_general(left, own, NT, preferred_element_type=jnp.float32)

    def step(k, carry):
        @pl.when(k < blocks)
        def _():
            forward(k)

        @pl.when((k >= LAG) & (k < blocks + LAG))
        def _():
            pass_on(k - LAG)

        @pl.when(k >= LAG + 2)
        def _():
            multiply(k - LAG - 2)

        return carry

    lax.fori_loop(0, blocks + LAG + 2, step, 0)
    for d in range(blocks):
        if d != middle:
            across(d).wait_send()
        for c in range(1, chips):
            hop(d, c).wait_send()
        for c in range(chips):
            hand(d, c).wait_send()


def write_kernel(members, kinds, n_mem, dep_row, acc, gram, depart, rows, lines, out, out_dep, sems):
    size = members * kinds
    total = size * n_mem
    every = members * n_mem
    tiles = -(-size // LANE)
    copies = []
    done = 0
    for first in range(0, every, GROUP):
        count = min(GROUP, every - first)
        for t in range(tiles):
            wide = min(LANE, size - t * LANE)
            for l in range(kinds):
                at = l * every + first
                to = pl.ds(first * kinds + l, count, stride=kinds)
                rows[t, to, 0:wide] = acc[at : at + count, t * LANE : t * LANE + wide]
        filled = (first + count) * kinds
        while done < total and min(done + LANE, total) <= filled:
            at = slice(done, min(total, done + LANE))
            i, tall = done // LANE, at.stop - done
            turned = [rows[t, at, :].T[: min(LANE, size - t * LANE)] for t in range(tiles)]
            turned = jnp.concatenate(turned, axis=0)
            for k in range(kinds):
                part = turned[k * members : (k + 1) * members]
                lines[i, pl.ds(k, members, stride=kinds), 0:tall] = part
            out[0, :, at] = lines[i, :, 0:tall]
            copy = pltpu.make_async_copy(out.at[:, :, at], gram.at[:, :, at], sems.at[1 + i])
            copy.start()
            copies.append(copy)
            done += LANE
        if first == 0:
            row, col = iota((size, size), 0), iota((size, size), 1)
            swap = jnp.where(col == (row % members) * kinds + row // members, 1.0, 0.0)
            out_dep[...] = jnp.dot(
                acc[dep_row : dep_row + 1, :], swap, precision=lax.Precision.HIGHEST,
                preferred_element_type=jnp.float32,
            )
            copies.append(pltpu.make_async_copy(out_dep, depart, sems.at[0]))
            copies[-1].start()
    for copy in copies:
        copy.wait()


def local(
    profiles, jacobian, departure, obs_rinv, obs_level, vertical_modes, send_rows, counts, loc_taper
):
    cols, members, levels = profiles.shape
    channels = jacobian.shape[1]
    blocks, capacity = send_rows.shape[1], send_rows.shape[2]
    kinds = vertical_modes.shape[1]
    n_mem = lax.axis_size("mem")
    chips = n_mem // 2
    share = -(-(kinds + 1) // n_mem)
    height = members + share
    size = members * kinds
    lanes = GROUP * channels
    dma = pltpu.SemaphoreType.DMA
    args = (
        profiles.transpose(1, 0, 2), jacobian.transpose(2, 1, 0),
        departure[None], obs_rinv[None], obs_level[None], vertical_modes.T,
        send_rows.transpose(1, 0, 2), counts, loc_taper.transpose(1, 0, 2),
    )
    args = [pltpu.with_memory_space_constraint(a, pltpu.MemorySpace.HBM) for a in args]
    buffers = [pltpu.VMEM(a.shape, a.dtype) for a in args]
    buffers[7] = pltpu.SMEM(counts.shape, counts.dtype)
    pitch = -(-levels // LANE) * LANE + 1
    acc_rows = size * n_mem + GROUP
    acc = pl.pallas_call(
        functools.partial(gather_kernel, members, kinds, share),
        out_shape=jax.ShapeDtypeStruct((acc_rows, size), jnp.float32),
        in_specs=[HBM] * 9,
        out_specs=VMEM,
        scratch_shapes=[
            *buffers,
            pltpu.VMEM((share * n_mem + SUB, levels), jnp.float32),
            pltpu.VMEM((cols // LANE, pitch * channels, LANE), jnp.float32),
            pltpu.VMEM((channels, cols, levels), jnp.bfloat16),
            pltpu.VMEM((cols // GROUP * SUB, lanes), jnp.float32),
            pltpu.VMEM((cols // GROUP, height, lanes), jnp.bfloat16),
            pltpu.VMEM((blocks, height, capacity), jnp.bfloat16),
            pltpu.VMEM((blocks, n_mem, height, capacity), jnp.bfloat16),
            dma((9,)), dma((blocks, chips)), dma((blocks, chips)), dma((blocks, chips)), dma((blocks, chips)),
        ],
        compiler_params=pltpu.CompilerParams(
            collective_id=0, has_side_effects=True, vmem_limit_bytes=32 << 20
        ),
        name="gather",
    )(*args)
    dep_row = size * n_mem + SUB - share + kinds % share
    total = size * n_mem
    gram, depart = pl.pallas_call(
        functools.partial(write_kernel, members, kinds, n_mem, dep_row),
        out_shape=(
            jax.ShapeDtypeStruct((1, size, total), jnp.float32),
            jax.ShapeDtypeStruct((1, size), jnp.float32),
        ),
        in_specs=[VMEM],
        out_specs=(HBM, HBM),
        scratch_shapes=[
            pltpu.VMEM((-(-size // LANE), total, LANE), jnp.float32),
            pltpu.VMEM((-(-total // LANE), size, LANE), jnp.float32),
            pltpu.VMEM((1, size, total), jnp.float32),
            pltpu.VMEM((1, size), jnp.float32),
            dma((1 + -(-total // LANE),)),
        ],
        compiler_params=pltpu.CompilerParams(vmem_limit_bytes=16 << 20),
        name="write",
    )(acc)
    return gram, depart


def solution(mesh):
    in_specs = (
        P("reg", "mem", None),
        P("reg", None, None),
        P("reg"),
        P("reg"),
        P("reg"),
        P(),
        P("reg", None, None),
        P("reg", None),
        P("reg", None, None),
    )
    out_specs = (P("reg", "mem", None), P("reg", "mem"))
    return jax.shard_map(local, mesh=mesh, in_specs=in_specs, out_specs=out_specs, check_vma=False)
```

```python
import functools

import jax
import jax.numpy as jnp
from jax import lax
from jax.experimental import pallas as pl
from jax.experimental.pallas import tpu as pltpu
from jax.sharding import PartitionSpec as P

ENS = 80
LANE = 128
SUB = 8
GROUP = 16
CROSS_REG = False
CROSS_HOP = True
LAG = 4
NT = (((1,), (1,)), ((), ()))
VMEM = pl.BlockSpec(memory_space=pltpu.VMEM)
HBM = pl.BlockSpec(memory_space=pltpu.MemorySpace.HBM)
MESH = pl.DeviceIdType.MESH


def iota(shape, dim):
    return lax.broadcasted_iota(jnp.int32, shape, dim)


def hot(mask):
    return jnp.where(mask, 1.0, 0.0).astype(jnp.bfloat16)


def times(left, right):
    return jnp.dot(left, right, preferred_element_type=jnp.float32)


def merge(a, b, bit, s, u):
    up = pltpu.roll(a, SUB - bit, 0)
    if b is None:
        return jnp.where((u & bit) != 0, up, a)
    low = (s & bit) == 0
    if 2 * bit == SUB:
        same = (s & bit) == (u & bit)
        return jnp.where(same, jnp.where(low, a, b), pltpu.roll(jnp.where(low, b, a), bit, 0))
    down = pltpu.roll(b, bit, 0)
    return jnp.where((u & bit) != 0, jnp.where(low, up, b), jnp.where(low, a, down))


def diagonal(parts, s, u):
    fours = [merge(parts[i], parts[i + 4] if len(parts) > 4 else None, 4, s, u) for i in range(4)]
    twos = [merge(fours[i], fours[i + 2], 2, s, u) for i in range(2)]
    return merge(twos[0], twos[1], 1, s, u)


def turn_jacobian(jac, wide, turned):
    levels, channels, cols = jac.shape
    pitch = wide.shape[1] // channels
    for l in range(levels):
        line = jac[l].astype(jnp.float32)
        for half in range(cols // LANE):
            for q in range(0, channels, SUB):
                part = line[q : q + SUB, half * LANE : (half + 1) * LANE]
                wide[half, pl.ds(q * pitch + l, SUB, stride=pitch), :] = part
    for half in range(cols // LANE):
        for q in range(channels):
            plane = wide[half, q * pitch : q * pitch + LANE, :]
            turned[q, half * LANE : (half + 1) * LANE, :] = plane.T[:, :levels].astype(jnp.bfloat16)


def side_rows(me, rinv, dep, level, modes, padded, extra, share):
    kinds, levels = modes.shape
    lanes = extra.shape[1]
    padded[...] = jnp.zeros_like(padded)
    padded[share : share + kinds, :] = modes[...] * ((ENS - 1) ** (-0.5))
    mine = padded[pl.ds(me * share, SUB), :].astype(jnp.bfloat16)
    s = iota((SUB, lanes), 0)
    holds_dep = (s == SUB - share + kinds % share) & (me == kinds // share)
    for g in range(extra.shape[0] // SUB):
        at = slice(g * lanes, (g + 1) * lanes)
        root = jnp.sqrt(rinv[:, at])
        high = root.astype(jnp.bfloat16).astype(jnp.float32)
        found = times(mine, hot(iota((levels, lanes), 0) == level[:, at]))
        found = jnp.where(holds_dep, dep[:, at] * root, found)
        found = jnp.where(s == 0, high, jnp.where(s == 1, root - high, found))
        extra[g * SUB : (g + 1) * SUB, :] = found
    channels = lanes // GROUP
    source, target = iota((lanes, lanes), 0), iota((lanes, lanes), 1)
    swap = hot(target == (source % channels) * GROUP + source // channels)
    extra[...] = times(extra[...].astype(jnp.bfloat16), swap)


def fill_table(prof, turned, extra, table):
    members, cols, levels = prof.shape
    groups, height, lanes = table.shape
    s, lane = iota((SUB, lanes), 0), iota((SUB, lanes), 1)
    u = lane % SUB
    upper = (lane // SUB) % 2 == 1

    def fill(g, carry):
        first = pl.ds(pl.multiple_of(g * GROUP, GROUP), GROUP)
        left = prof[:, first, :].reshape(members * GROUP, levels)
        right = turned[:, first, :].reshape(lanes, levels)
        full = lax.dot_general(left, right, NT, preferred_element_type=jnp.float32)
        parts = []
        for m in range(members):
            x = m * GROUP
            parts.append(jnp.where(upper, full[x + SUB : x + 2 * SUB], full[x : x + SUB]))
        more = extra[pl.ds(pl.multiple_of(g * SUB, SUB), SUB), :]
        root = more[0:1] + more[1:2]
        rows = [diagonal(parts[m : m + SUB], s, u) * root for m in range(0, members, SUB)]
        rows[-1] = jnp.where(s < members % SUB, rows[-1], more)
        table[g] = jnp.concatenate(rows, axis=0).astype(jnp.bfloat16)
        return carry

    lax.fori_loop(0, groups, fill, 0, unroll=16)


def gather_kernel(
    members, kinds, share, prof_h, jac_h, dep_h, rinv_h, level_h, modes_h, rows_h, counts_h, taper_h, acc,
    prof, jac, dep, rinv, level, modes, rows, counts, taper,
    padded, wide, turned, extra, table, mine, region,
    s_in, s_reg, r_reg, s_hand, r_hand,
):
    blocks, height, capacity = mine.shape
    middle = blocks // 2
    n_mem, n_reg = lax.axis_size("mem"), lax.axis_size("reg")
    me, reg = lax.axis_index("mem"), lax.axis_index("reg")
    chips = n_mem // 2
    groups, _, lanes = table.shape
    channels = lanes // GROUP
    partner = {"mem": me + 1 - 2 * (me % 2), "reg": reg}
    pairs = [
        (level_h, level), (modes_h, modes), (rinv_h, rinv), (dep_h, dep), (rows_h, rows),
        (counts_h, counts), (taper_h, taper), (jac_h, jac), (prof_h, prof),
    ]
    loads = [pltpu.make_async_copy(h, v, s_in.at[i]) for i, (h, v) in enumerate(pairs)]
    for load in loads:
        load.start()

    def other(x):
        return x + 1 - 2 * lax.rem(x, 2)

    def target(d):
        to = lax.rem(reg + d - middle + n_reg, n_reg)
        return {"mem": other(me) if CROSS_REG else me, "reg": to}

    def peer(c):
        to = lax.rem(me + 2 * c, n_mem)
        return other(to) if CROSS_HOP else to

    def near(d, device):
        return jnp.where(d == middle, device, other(device)) if CROSS_REG else device

    def far(d, c):
        return near(d, peer(chips - c))

    def remote(src, dst, send, recv, device):
        return pltpu.make_async_remote_copy(
            src_ref=src, dst_ref=dst, send_sem=send, recv_sem=recv,
            device_id=device, device_id_type=MESH,
        )

    def across(d):
        return remote(mine.at[d], region.at[d, me], s_reg.at[d, 0], r_reg.at[d, 0], target(d))

    def hop(d, c):
        at = region.at[d, near(d, me)]
        to = {"mem": peer(c), "reg": reg}
        return remote(at, at, s_reg.at[d, c], r_reg.at[d, c], to)

    def hand(d, c):
        at = region.at[d, near(d, me) if c == 0 else far(d, c)]
        return remote(at, at, s_hand.at[d, c], r_hand.at[d, c], partner)

    def spread_out(d):
        for c in range(1, chips):
            hop(d, c).start()
        hand(d, 0).start()

    barrier = pltpu.get_barrier_semaphore()
    greeted = [target(d) for d in range(blocks) if d != middle]
    greeted += [partner] + [{"mem": peer(c), "reg": reg} for c in range(1, chips)]
    for device in greeted:
        pl.semaphore_signal(barrier, inc=1, device_id=device, device_id_type=MESH)

    at = lax.rem(middle - reg + n_reg, n_reg)
    lead = jnp.where(at < blocks, at, 0)

    def sent(k):
        return lax.rem(lead + jnp.where(2 * reg < n_reg, jnp.where(k < 2, k, blocks + 1 - k), k), blocks)

    late = 4 * reg >= 3 * n_reg

    home = lax.rem(middle - lead + blocks, blocks)

    def taken(k):
        first = jnp.where(k == 0, home, jnp.where(k <= home, k - 1, k))
        return blocks - 1 - lax.rem(lead + jnp.where(late, blocks - 1 - k, first), blocks)

    for load in loads[:4]:
        load.wait()
    side_rows(me, rinv, dep, level, modes, padded, extra, share)
    for load in loads[4:7]:
        load.wait()

    def placed(d):
        live = iota((1, capacity), 1) < counts[0, d]
        return live, jnp.where(live, rows[d], 0)

    loads[7].wait()
    turn_jacobian(jac, wide, turned)
    loads[8].wait()
    fill_table(prof, turned, extra, table)

    s = iota((height, capacity), 0)
    is_dep = (s == members + kinds % share) & (me == kinds // share)
    for k in range(blocks):
        d = sent(k)
        live, picked = placed(d)
        high = picked // lanes
        low = (picked % channels) * GROUP + (picked // channels) % GROUP
        found = times(table[...].reshape(groups * height, lanes), hot(iota((lanes, capacity), 0) == low))
        chosen = found[:height]
        for h in range(1, groups):
            chosen = jnp.where(high == h, found[h * height : (h + 1) * height], chosen)
        root = jnp.sqrt(jnp.where(live, taper[d], 0.0))
        block = (chosen * jnp.where((s < members) | is_dep, root, 1.0)).astype(jnp.bfloat16)
        mine[d] = block
        if k == 0:
            pl.semaphore_wait(barrier, len(greeted))

        @pl.when(d == middle)
        def _():
            region[middle, me] = block
            spread_out(middle)

        @pl.when(d != middle)
        def _():
            across(d).start()

    acc[...] = jnp.zeros_like(acc)
    rows_of_eight = iota((SUB, capacity), 0)

    def joined(first, second, rolled=False):
        if not rolled:
            second = pltpu.roll(second, share, 0)
        seam = jnp.where(rows_of_eight < SUB - share, first[height - SUB :], second[:SUB])
        return jnp.concatenate([first[: height - SUB], seam, second[SUB:]], axis=0)

    def forward(k):
        d = taken(k)

        @pl.when(d != middle)
        def _():
            across(d).wait_recv()
            spread_out(d)

    def pass_on(k):
        d = taken(k)
        for c in range(1, chips):
            hop(d, c).wait_recv()
            hand(d, c).start()

    def multiply(k):
        d = taken(k)
        for c in range(chips):
            hand(d, c).wait_recv()
        parts = [region[d, j].astype(jnp.float32) for j in range(n_mem)]
        every = [joined(parts[j], parts[j + 1]) for j in range(0, n_mem, 2)]
        every = jnp.concatenate(every, axis=0).astype(jnp.bfloat16)
        low = region[d, me].astype(jnp.float32)
        high = pltpu.roll(low, share, 0)
        lines = []
        for l in range(kinds):
            at = members + l % share
            lines.append(parts[l // share][at : at + 1])
        own = []
        for l in range(0, kinds, 2):
            own.append(joined(low * lines[l], high * lines[l + 1], True))
        own = jnp.concatenate(own, axis=0).astype(jnp.bfloat16)
        left = []
        for line in lines:
            tall = jnp.broadcast_to(line, (GROUP, capacity)).astype(jnp.bfloat16)
            left.append(every * jnp.concatenate([tall] * (every.shape[0] // GROUP), axis=0))
        last = parts[kinds // share][height - SUB :]
        left.append(jnp.concatenate([last, last], axis=0).astype(jnp.bfloat16))
        left = jnp.concatenate(left, axis=0)
        acc[...] += lax.dot_general(left, own, NT, preferred_element_type=jnp.float32)

    def step(k, carry):
        @pl.when(k < blocks)
        def _():
            forward(k)

        @pl.when((k >= LAG) & (k < blocks + LAG))
        def _():
            pass_on(k - LAG)

        @pl.when(k >= LAG + 2)
        def _():
            multiply(k - LAG - 2)

        return carry

    lax.fori_loop(0, blocks + LAG + 2, step, 0)
    for d in range(blocks):
        if d != middle:
            across(d).wait_send()
        for c in range(1, chips):
            hop(d, c).wait_send()
        for c in range(chips):
            hand(d, c).wait_send()


def write_kernel(members, kinds, n_mem, dep_row, acc, gram, depart, rows, lines, out, out_dep, sems):
    size = members * kinds
    total = size * n_mem
    every = members * n_mem
    tiles = -(-size // LANE)
    copies = []
    done = 0
    for first in range(0, every, GROUP):
        count = min(GROUP, every - first)
        for t in range(tiles):
            wide = min(LANE, size - t * LANE)
            for l in range(kinds):
                at = l * every + first
                to = pl.ds(first * kinds + l, count, stride=kinds)
                rows[t, to, 0:wide] = acc[at : at + count, t * LANE : t * LANE + wide]
        filled = (first + count) * kinds
        while done < total and min(done + LANE, total) <= filled:
            at = slice(done, min(total, done + LANE))
            i, tall = done // LANE, at.stop - done
            turned = [rows[t, at, :].T[: min(LANE, size - t * LANE)] for t in range(tiles)]
            turned = jnp.concatenate(turned, axis=0)
            for k in range(kinds):
                part = turned[k * members : (k + 1) * members]
                lines[i, pl.ds(k, members, stride=kinds), 0:tall] = part
            out[0, :, at] = lines[i, :, 0:tall]
            copy = pltpu.make_async_copy(out.at[:, :, at], gram.at[:, :, at], sems.at[1 + i])
            copy.start()
            copies.append(copy)
            done += LANE
        if first == 0:
            row, col = iota((size, size), 0), iota((size, size), 1)
            swap = jnp.where(col == (row % members) * kinds + row // members, 1.0, 0.0)
            out_dep[...] = jnp.dot(
                acc[dep_row : dep_row + 1, :], swap, precision=lax.Precision.HIGHEST,
                preferred_element_type=jnp.float32,
            )
            copies.append(pltpu.make_async_copy(out_dep, depart, sems.at[0]))
            copies[-1].start()
    for copy in copies:
        copy.wait()


def local(
    profiles, jacobian, departure, obs_rinv, obs_level, vertical_modes, send_rows, counts, loc_taper
):
    cols, members, levels = profiles.shape
    channels = jacobian.shape[1]
    blocks, capacity = send_rows.shape[1], send_rows.shape[2]
    kinds = vertical_modes.shape[1]
    n_mem = lax.axis_size("mem")
    chips = n_mem // 2
    share = -(-(kinds + 1) // n_mem)
    height = members + share
    size = members * kinds
    lanes = GROUP * channels
    dma = pltpu.SemaphoreType.DMA
    args = (
        profiles.transpose(1, 0, 2), jacobian.transpose(2, 1, 0),
        departure[None], obs_rinv[None], obs_level[None], vertical_modes.T,
        send_rows.transpose(1, 0, 2), counts, loc_taper.transpose(1, 0, 2),
    )
    args = [pltpu.with_memory_space_constraint(a, pltpu.MemorySpace.HBM) for a in args]
    buffers = [pltpu.VMEM(a.shape, a.dtype) for a in args]
    buffers[7] = pltpu.SMEM(counts.shape, counts.dtype)
    pitch = -(-levels // LANE) * LANE + 1
    acc_rows = size * n_mem + GROUP
    acc = pl.pallas_call(
        functools.partial(gather_kernel, members, kinds, share),
        out_shape=jax.ShapeDtypeStruct((acc_rows, size), jnp.float32),
        in_specs=[HBM] * 9,
        out_specs=VMEM,
        scratch_shapes=[
            *buffers,
            pltpu.VMEM((share * n_mem + SUB, levels), jnp.float32),
            pltpu.VMEM((cols // LANE, pitch * channels, LANE), jnp.float32),
            pltpu.VMEM((channels, cols, levels), jnp.bfloat16),
            pltpu.VMEM((cols // GROUP * SUB, lanes), jnp.float32),
            pltpu.VMEM((cols // GROUP, height, lanes), jnp.bfloat16),
            pltpu.VMEM((blocks, height, capacity), jnp.bfloat16),
            pltpu.VMEM((blocks, n_mem, height, capacity), jnp.bfloat16),
            dma((9,)), dma((blocks, chips)), dma((blocks, chips)), dma((blocks, chips)), dma((blocks, chips)),
        ],
        compiler_params=pltpu.CompilerParams(
            collective_id=0, has_side_effects=True, vmem_limit_bytes=32 << 20
        ),
        name="gather",
    )(*args)
    dep_row = size * n_mem + SUB - share + kinds % share
    total = size * n_mem
    gram, depart = pl.pallas_call(
        functools.partial(write_kernel, members, kinds, n_mem, dep_row),
        out_shape=(
            jax.ShapeDtypeStruct((1, size, total), jnp.float32),
            jax.ShapeDtypeStruct((1, size), jnp.float32),
        ),
        in_specs=[VMEM],
        out_specs=(HBM, HBM),
        scratch_shapes=[
            pltpu.VMEM((-(-size // LANE), total, LANE), jnp.float32),
            pltpu.VMEM((-(-total // LANE), size, LANE), jnp.float32),
            pltpu.VMEM((1, size, total), jnp.float32),
            pltpu.VMEM((1, size), jnp.float32),
            dma((1 + -(-total // LANE),)),
        ],
        compiler_params=pltpu.CompilerParams(vmem_limit_bytes=16 << 20),
        name="write",
    )(acc)
    return gram, depart


def solution(mesh):
    in_specs = (
        P("reg", "mem", None),
        P("reg", None, None),
        P("reg"),
        P("reg"),
        P("reg"),
        P(),
        P("reg", None, None),
        P("reg", None),
        P("reg", None, None),
    )
    out_specs = (P("reg", "mem", None), P("reg", "mem"))
    return jax.shard_map(local, mesh=mesh, in_specs=in_specs, out_specs=out_specs, check_vma=False)
```
